256 devices in a mesh: dp: 128 (over x, y_lo, z, core), rep: 2 (over y_hi).
Axes of the slice: x: 4, y: 4 (y_hi: 2, y_lo: 2; y = y_hi * 2 + y_lo), z: 8, core: 2. Of those that a mesh axis runs over, the one named last changes fastest.
Arguments:
- images: bfloat16 [131072, 512], P(('dp', 'rep')), may hold values from -6 to 6
- text_feats: bfloat16 [131072, 768], P(('dp', 'rep')), may hold values from -24 to 24
- text_proj: bfloat16 [768, 512], replicated, may hold values from -0.21875 to 0.21875
- logit_scale: float32 [1], replicated, may hold values from 4 to 16
- logit_bias: float32 [1], replicated, may hold values from -6 to -2
Outputs:
- image_grad: bfloat16 [131072, 512], P(('dp', 'rep'))
- proj_grad: float32 [768, 512], P(('dp', 'rep'))
The draws below stay inside these ranges and needn't reach their ends.
All inputs are finite; a program needn't handle non-finite values.
Results may differ from the reference program's by a relative error of at most 0.013.
Values may be sent and summed in bfloat16 or wider, within the bound.
No kernel may reach another device: no remote copies, remote signals or barrier semaphores. Data moves between devices by JAX's collectives and lax.ppermute only.
A program may use at most 64 MiB of HBM per device.

```python
import math
import jax
import jax.numpy as jnp
from jax import lax

E = 512
D_TEXT = 768
ROWS = 512
SHIFTS = 8
BATCH = 131072
N_DP = 128
N_REP = 2


def strengthened(values, rng, source, target, blocks, factor):
    owner, partner = [(jnp.arange(values.shape[position]) // (values.shape[position] // blocks)).reshape([-1 if axis == position else 1 for axis in range(values.ndim)]) for position in (source, target)]
    chosen = jax.random.permutation(rng, blocks)[partner]
    strong = (owner == chosen) | (owner == (partner + blocks // 2) % blocks)
    return jnp.where(strong, factor * values, values)


def level_of(own_key, shape, shards, low, high):
    level = 1.0
    for dim, blocks in shards:
        draws = jax.random.uniform(jax.random.fold_in(jax.random.fold_in(own_key, 6), dim), (blocks,), jnp.float32, low / len(shards), high / len(shards))
        level = level * jnp.repeat(jnp.exp(draws), shape[dim] // blocks).reshape((-1,) + (1,) * (len(shape) - 1 - dim))
    return level


def gaussian(stream_key, shape, scale, limit, cuts=(), kind=jnp.bfloat16):
    values = scale * jax.random.normal(stream_key, shape, jnp.float32)
    if cuts:
        values = values * level_of(stream_key, shape, cuts, -0.22, 0.18)
    return jnp.clip(values, -limit, limit).astype(kind)


def bell_draw_with(rng, dims, width, bound, shards, heavy, kind=jnp.bfloat16):
    values = width * jax.random.normal(rng, dims, jnp.float32)
    if shards:
        values = values * level_of(rng, dims, shards, -0.22, 0.18)
    return jnp.clip(strengthened(values, jax.random.fold_in(rng, 3), *heavy), -bound, bound).astype(kind)


def setup_inputs(seed: int = 0) -> dict:
    keys = jax.random.split(jax.random.key(seed), 6)
    images = gaussian(keys[0], (BATCH, E), 1.0, 6.0, ((0, 256),))
    text_feats = bell_draw_with(keys[1], (BATCH, D_TEXT), 1.0, 24.0, ((0, 256),), (0, 1, 256, 6.0))
    text_proj = gaussian(keys[2], (D_TEXT, E), D_TEXT ** -0.5, 0.21875)
    logit_scale = jnp.clip(jnp.exp(jax.random.uniform(keys[3], (1,), jnp.float32, math.log(4.0), math.log(16.0))), 4.0, 16.0)
    logit_bias = jnp.clip(jax.random.uniform(keys[4], (1,), jnp.float32, -6.0, -2.0), -6.0, -2.0)
    return {"images": images, "text_feats": text_feats, "text_proj": text_proj, "logit_scale": logit_scale, "logit_bias": logit_bias}


EPS = 1e-06

def unit_rows(values):
    square = lax.optimization_barrier(jnp.sum(values * values, axis=-1, keepdims=True))
    factor = lax.rsqrt(square + EPS)
    return (values * factor, factor)

def back_rows(normal, factor, upstream):
    return factor * (upstream - normal * lax.optimization_barrier(jnp.sum(normal * upstream, axis=-1, keepdims=True)))

def reference(images, text_feats, text_proj, logit_scale, logit_bias):
    blocks = N_DP * N_REP
    image_unit, image_factor = unit_rows(images.astype(jnp.float32))
    u_round = lax.optimization_barrier(image_unit.astype(jnp.bfloat16))
    text_raw = jnp.dot(text_feats, text_proj, preferred_element_type=jnp.float32)
    text_unit, text_factor = unit_rows(text_raw)
    v_round = lax.optimization_barrier(text_unit.astype(jnp.bfloat16))
    u_blocks = u_round.astype(jnp.float32).reshape(blocks, ROWS, E)
    v_blocks = v_round.astype(jnp.float32).reshape(blocks, ROWS, E)
    scaling = logit_scale[0]
    shifted = logit_bias[0]
    positions = jnp.arange(ROWS, dtype=jnp.int32)
    identity_mask = (positions[:, None] == positions[None, :]).astype(jnp.float32)
    image_sum = jnp.zeros((blocks, ROWS, E), jnp.float32)
    text_sum = jnp.zeros((blocks, ROWS, E), jnp.float32)
    for offset in range(SHIFTS + 1):
        held = jnp.roll(v_blocks, offset * N_REP, axis=0)
        logits = scaling * jnp.einsum('brd,bcd->brc', u_blocks, held) + shifted
        if offset == 0:
            label = 2.0 * identity_mask - 1.0
        else:
            label = -jnp.ones((ROWS, ROWS), jnp.float32)
        weighted = scaling * -label * jax.nn.sigmoid(-label * logits)
        weighted = lax.optimization_barrier(weighted.astype(jnp.bfloat16)).astype(jnp.float32)
        image_sum = image_sum + jnp.einsum('brc,bcd->brd', weighted, held)
        returned = jnp.einsum('brc,brd->bcd', weighted, u_blocks)
        text_sum = text_sum + jnp.roll(returned, -offset * N_REP, axis=0)
    image_grad = back_rows(image_unit, image_factor, image_sum.reshape(-1, E)).astype(jnp.bfloat16)
    text_grad = back_rows(text_unit, text_factor, text_sum.reshape(-1, E)).astype(jnp.bfloat16)
    proj_grad = lax.dot_general(text_feats, text_grad, (((0,), (0,)), ((), ())), preferred_element_type=jnp.float32)
    return (image_grad, proj_grad)
```

```python
import jax
import jax.numpy as jnp
from jax import lax
from jax.sharding import Mesh, PartitionSpec as P

EPS = 1e-06
SHIFTS = 8
PIECES = 2
AXES = ("x", "yl", "z", "c", "yh")
DP = ("x", "yl", "z", "c")
CHIPS = ("x", "yl", "z", "yh")
SIZES = (4, 2, 8, 2, 2)


def unit_rows(values):
    square = jnp.sum(values * values, axis=-1, keepdims=True)
    factor = lax.rsqrt(square + EPS)
    return (values * factor, factor)


def back_rows(normal, factor, upstream):
    return factor * (upstream - normal * jnp.sum(normal * upstream, axis=-1, keepdims=True))


def next_chip(block):
    chips = lax.axis_size(DP) // 2
    route = [(2 * i + c, 2 * ((i + (1, -1)[c]) % chips) + c) for i in range(chips) for c in (0, 1)]
    return lax.ppermute(block, DP, route)


def other_core(block):
    return lax.ppermute(block, "c", [(0, 1), (1, 0)])


def on_device(images, text_feats, text_proj, logit_scale, logit_bias):
    core = lax.axis_index("c")
    first = core == 0
    rows = images.shape[0]
    bf16, f32 = jnp.bfloat16, jnp.float32
    scaling, shifted = logit_scale[0], logit_bias[0]

    images_raw = images.astype(f32)
    text_raw = jnp.dot(text_feats, text_proj, preferred_element_type=f32)
    image_unit, image_factor = unit_rows(images_raw)
    text_unit, text_factor = unit_rows(text_raw)
    u_round = image_unit.astype(bf16)
    v_round = text_unit.astype(bf16)

    stream_own = jnp.where(first, v_round, u_round)
    still_own = jnp.where(first, u_round, v_round)
    stream_sib = other_core(still_own)
    raw_sib = other_core(jnp.where(first, text_raw, images_raw))
    feats_sib = other_core(text_feats)
    unit_own = jnp.where(first, image_unit, text_unit)
    factor_own = jnp.where(first, image_factor, text_factor)
    unit_sib, factor_sib = unit_rows(raw_sib)
    still_sib = unit_sib.astype(bf16)

    def weigh(still, held, row0):
        logits = (
            scaling
            * lax.dot_general(still, held, (((1,), (1,)), ((), ())), preferred_element_type=f32)
            + shifted
        )
        if row0 is None:
            return (scaling * jax.nn.sigmoid(logits)).astype(bf16)
        r = lax.broadcasted_iota(jnp.int32, logits.shape, 0)
        q = lax.broadcasted_iota(jnp.int32, logits.shape, 1) + row0
        label = jnp.where(r == q, 1.0, -1.0).astype(f32)
        return (scaling * -label * jax.nn.sigmoid(-label * logits)).astype(bf16)

    def term(still, held, row0=None):
        return jnp.dot(weigh(still, held, row0), held, preferred_element_type=f32)

    step = rows // PIECES
    cut = lambda b: [b[i * step : (i + 1) * step] for i in range(PIECES)]
    held_own, held_sib = cut(stream_own), cut(stream_sib)
    moving_own = [next_chip(b) for b in held_own]
    moving_sib = [next_chip(b) for b in held_sib]
    sum_own = sum_sib = 0.0
    for i in range(PIECES):
        sum_own = sum_own + term(still_own, held_own[i], i * step)
        sum_sib = sum_sib + term(still_sib, held_own[i])
    for i in range(PIECES):
        sum_sib = sum_sib + term(still_sib, held_sib[i], i * step)
    last = SHIFTS // 2
    for hop in range(1, last + 1):
        held_own, held_sib = moving_own, moving_sib
        if hop < last:
            moving_own = [next_chip(b) for b in held_own]
            moving_sib = [next_chip(b) for b in held_sib]
        for b in held_own:
            sum_own = sum_own + term(still_own, b)
            if hop < last:
                sum_sib = sum_sib + term(still_sib, b)
        for b in held_sib:
            sum_own = sum_own + term(still_own, b)
            sum_sib = sum_sib + term(still_sib, b)

    grads = jnp.concatenate(
        [back_rows(unit_own, factor_own, sum_own), back_rows(unit_sib, factor_sib, sum_sib)]
    ).astype(bf16)
    crossed = other_core(grads)
    image_grad = jnp.where(first, grads[:rows], crossed[rows:])
    text_grads = jnp.where(first, crossed, grads)
    feats = jnp.concatenate(
        [jnp.where(first, feats_sib, text_feats), jnp.where(first, text_feats, feats_sib)]
    )

    chips = 128
    wide = text_feats.shape[1]
    per = wide // (2 * chips)
    at = lax.broadcasted_iota(jnp.int32, (wide, per * chips), 1)
    chip, j = at % chips, at // chips
    owner = (chip // 2) * 4 + core * 2 + chip % 2
    pick = (lax.broadcasted_iota(jnp.int32, (wide, per * chips), 0) == owner * per + j).astype(bf16)
    picked = jnp.dot(feats, pick, preferred_element_type=f32).astype(bf16)
    part = lax.dot_general(picked, text_grads, (((0,), (0,)), ((), ())), preferred_element_type=f32)
    part = part.astype(bf16).reshape(per, chips, -1)
    spread = lax.all_to_all(part, CHIPS, 1, 0, tiled=True)
    proj_grad = jnp.sum(spread.reshape(chips, per, -1).astype(f32), axis=0)
    return (image_grad, proj_grad)


def solution(mesh):
    fine = Mesh(mesh.devices.reshape(SIZES), AXES)
    split = P(AXES, None)
    in_specs = (split, split, P(), P(), P())
    return jax.shard_map(
        on_device, mesh=fine, in_specs=in_specs, out_specs=(split, split), check_vma=False
    )
```

```python
import functools

import jax
import jax.numpy as jnp
from jax import lax
from jax.experimental import pallas as pl
from jax.experimental.pallas import tpu as pltpu
from jax.sharding import Mesh, PartitionSpec as P

EPS = 1e-06
SHIFTS = 8
PIECE = 256
AXES = ("x", "yl", "z", "c", "yh")
DP = ("x", "yl", "z", "c")
PLANE = ("x", "yl", "yh")
SIZES = (4, 2, 8, 2, 2)
BF16, F32 = jnp.bfloat16, jnp.float32
SCALARS = pl.BlockSpec(memory_space=pltpu.SMEM)
LIMIT = pltpu.CompilerParams(vmem_limit_bytes=20 << 20)


def row_sum(values):
    return jnp.sum(values, axis=-1, keepdims=True)


def unit_rows(values):
    factor = lax.rsqrt(row_sum(values * values) + EPS)
    return (values * factor, factor)


def back_rows(normal, factor, upstream):
    return factor * (upstream - normal * row_sum(normal * upstream))


def next_chip(block):
    chips = lax.axis_size(DP) // 2
    route = [(2 * i + c, 2 * ((i + (1, -1)[c]) % chips) + c) for i in range(chips) for c in (0, 1)]
    return lax.ppermute(block, DP, route)


def other_core(block):
    return lax.ppermute(block, "c", [(0, 1), (1, 0)])


def cost(flops, nbytes):
    return pl.CostEstimate(flops=flops, bytes_accessed=nbytes, transcendentals=0)


def units_kernel(core_ref, image_ref, feats_ref, proj_ref, stream_ref, still_ref, own_ref, cross_ref):
    image = image_ref[...].astype(F32)
    text = jnp.dot(feats_ref[...], proj_ref[...], preferred_element_type=F32)
    u = unit_rows(image)[0].astype(BF16)
    v = unit_rows(text)[0].astype(BF16)

    @pl.when(core_ref[0] == 0)
    def _():
        stream_ref[...], still_ref[...] = v, u
        own_ref[...], cross_ref[...] = image, text

    @pl.when(core_ref[0] != 0)
    def _():
        stream_ref[...], still_ref[...] = u, v
        own_ref[...], cross_ref[...] = text, image


def units(core, images, feats, proj, part):
    width = proj.shape[1]
    shape = lambda dtype: jax.ShapeDtypeStruct((PIECE, width), dtype)
    pick = lambda array: pl.BlockSpec((PIECE, array.shape[1]), lambda i: (part, 0))
    out = pl.BlockSpec((PIECE, width), lambda i: (0, 0))
    return pl.pallas_call(
        units_kernel,
        grid=(1,),
        out_shape=[shape(BF16), shape(BF16), shape(F32), shape(F32)],
        in_specs=[SCALARS, pick(images), pick(feats), pl.BlockSpec(proj.shape, lambda i: (0, 0))],
        out_specs=[out] * 4,
        compiler_params=LIMIT,
        cost_estimate=cost(2 * PIECE * proj.shape[0] * width, 2 << 20),
        name=f"units{part}",
    )(core, images, feats, proj)


def term(scalars, still, held, offset=None):
    scale, bias = scalars[0], scalars[1]
    logits = lax.dot_general(still, held, (((1,), (1,)), ((), ())), preferred_element_type=F32)
    logits = scale * logits + bias
    if offset is None:
        weighted = scale / (1.0 + jnp.exp(-logits))
    else:
        rows = lax.broadcasted_iota(jnp.int32, logits.shape, 0)
        cols = lax.broadcasted_iota(jnp.int32, logits.shape, 1)
        label = jnp.where(rows + offset == cols, 1.0, -1.0)
        weighted = -label * scale / (1.0 + jnp.exp(label * logits))
    return jnp.dot(weighted.astype(BF16), held, preferred_element_type=F32)


def first_kernel(per, scalars, still_ref, *refs):
    held, out_ref = refs[:-1], refs[-1]
    i = pl.program_id(0)

    @pl.when(i < per)
    def _():
        out_ref[...] = sum(
            term(scalars, still_ref[...], held[j][...], (i - j) * PIECE) for j in range(per)
        )

    @pl.when(i >= per)
    def _():
        still = still_ref[...]
        out_ref[...] = sum(term(scalars, still, held[j][...]) for j in range(per)) + sum(
            term(scalars, still, held[per + j][...], (i - per - j) * PIECE) for j in range(per)
        )


def hop_kernel(scalars, still_ref, sums_ref, *refs):
    held, out_ref = refs[:-1], refs[-1]
    still = still_ref[...]
    out_ref[...] = sums_ref[...] + sum(term(scalars, still, h[...]) for h in held)


def last_kernel(scalars, still_ref, raw_ref, sums_ref, *refs):
    held, out_ref = refs[:-1], refs[-1]
    still = still_ref[...]
    upstream = sums_ref[...] + sum(term(scalars, still, h[...]) for h in held)
    normal, factor = unit_rows(raw_ref[...])
    out_ref[...] = back_rows(normal, factor, upstream).astype(BF16)


def tiles(kernel, scalars, streamed, held, dtype, blocks, alias=None, name=None):
    width = held[0].shape[1]
    row = pl.BlockSpec((PIECE, width), lambda i: (i, 0))
    whole = pl.BlockSpec((PIECE, width), lambda i: (0, 0))
    rows = streamed[0].shape[0]
    return pl.pallas_call(
        kernel,
        grid=(blocks,),
        out_shape=jax.ShapeDtypeStruct((rows, width), dtype),
        in_specs=[SCALARS] + [row] * len(streamed) + [whole] * len(held),
        out_specs=row,
        input_output_aliases={} if alias is None else {alias: 0},
        compiler_params=LIMIT,
        cost_estimate=cost(4 * len(held) * blocks * PIECE * PIECE * width, 6 << 20),
        name=name,
    )(scalars, *streamed, *held)


def proj_kernel(core_ref, feats_ref, mine_ref, crossed_ref, out_ref, sum_ref):
    i = pl.program_id(0)
    grads = jnp.where(core_ref[0] == 0, crossed_ref[...], mine_ref[...])
    part = lax.dot_general(
        feats_ref[...], grads, (((0,), (0,)), ((), ())), preferred_element_type=F32
    )

    @pl.when(i == 0)
    def _():
        sum_ref[...] = part

    @pl.when(i > 0)
    def _():
        sum_ref[...] += part

    @pl.when(i == pl.num_programs(0) - 1)
    def _():
        out_ref[...] = sum_ref[...].astype(BF16)


def proj_part(core, feats, mine, crossed):
    depth, rows = feats.shape
    width = mine.shape[1]
    block = lambda n: pl.BlockSpec((PIECE, n), lambda i: (i, 0))
    return pl.pallas_call(
        proj_kernel,
        grid=(depth // PIECE,),
        out_shape=jax.ShapeDtypeStruct((rows, width), BF16),
        in_specs=[SCALARS, block(rows), block(width), block(width)],
        out_specs=pl.BlockSpec((rows, width), lambda i: (0, 0)),
        scratch_shapes=[pltpu.VMEM((rows, width), F32)],
        compiler_params=LIMIT,
        cost_estimate=cost(2 * depth * rows * width, 3 << 20),
        name="proj",
    )(core, feats, mine, crossed)


def on_device(images, text_feats, text_proj, logit_scale, logit_bias):
    core_id = lax.axis_index("c").astype(jnp.int32)
    core = core_id.reshape(1)
    first = core_id == 0
    rows = images.shape[0]
    per = rows // PIECE
    scalars = jnp.concatenate([logit_scale, logit_bias])

    stream, still, raw, cross = zip(
        *(units(core, images, text_feats, text_proj, i) for i in range(per))
    )
    held = list(stream)
    moving = [next_chip(b) for b in held]
    sibling = [other_core(b) for b in still]
    held += sibling
    moving += [next_chip(b) for b in sibling]
    still = jnp.concatenate(still + tuple(other_core(b) for b in stream))
    raw = jnp.concatenate(raw + tuple(other_core(b) for b in cross))
    feats_sib = other_core(text_feats)

    sums = tiles(
        functools.partial(first_kernel, per), scalars, [still], held, F32, 2 * per, name="hop0"
    )
    last = SHIFTS // 2
    for hop in range(1, last):
        held = moving
        moving = [next_chip(b) for b in held]
        sums = tiles(hop_kernel, scalars, [still, sums], held, F32, 2 * per, 2, name=f"hop{hop}")
    sums = tiles(hop_kernel, scalars, [still, sums], moving[:per], F32, per, 2, name="hop4own")
    grads = tiles(
        last_kernel, scalars, [still, raw, sums], moving[per:], BF16, 2 * per, name="hop4sib"
    )

    feats = jnp.concatenate(
        [jnp.where(first, feats_sib, text_feats), jnp.where(first, text_feats, feats_sib)]
    )
    wide = text_feats.shape[1]
    deep, plane = lax.axis_size("z"), lax.axis_size(PLANE)
    each = wide // (2 * deep * plane)
    at = lax.broadcasted_iota(jnp.int32, (wide, wide // 2), 1)
    j, z, p = at % each, (at // each) % deep, at // (each * deep)
    owner = (((p // 2) * deep + z) * 2 + core_id) * 2 + p % 2
    pick = (lax.broadcasted_iota(jnp.int32, (wide, wide // 2), 0) == owner * each + j).astype(BF16)
    feats = jnp.dot(feats, pick, preferred_element_type=F32).astype(BF16)

    crossed = other_core(grads)
    part = proj_part(core, feats, grads, crossed)
    image_grad = jnp.where(first, grads[:rows], crossed[rows:])
    part = part.reshape(plane, deep * each, -1)
    part = lax.all_to_all(part, PLANE, 0, 0, tiled=True)
    part = jnp.sum(part.astype(F32), axis=0).reshape(deep, each, -1)
    part = lax.all_to_all(part, "z", 0, 0, tiled=True)
    return (image_grad, jnp.sum(part, axis=0))


def solution(mesh):
    fine = Mesh(mesh.devices.reshape(SIZES), AXES)
    split = P(AXES, None)
    in_specs = (split, split, P(), P(), P())
    return jax.shard_map(
        on_device, mesh=fine, in_specs=in_specs, out_specs=(split, split), check_vma=False
    )
```

```python
import functools

import jax
import jax.numpy as jnp
from jax import lax
from jax.experimental import pallas as pl
from jax.experimental.pallas import tpu as pltpu
from jax.sharding import Mesh, PartitionSpec as P


EPS = 1e-06
LOAD = 128
SHIFTS = 8
PIECE = 256
AXES = ("x", "yl", "z", "c", "yh")
DP = ("x", "yl", "z", "c")
PLANE = ("x", "yl", "yh")
SIZES = (4, 2, 8, 2, 2)
BF16, F32 = jnp.bfloat16, jnp.float32
CHIP = pl.BlockSpec(memory_space=pltpu.VMEM)
SCALARS = pl.BlockSpec(memory_space=pltpu.SMEM)
LIMIT = pltpu.CompilerParams(vmem_limit_bytes=20 << 20)


def row_sum(values):
    return jnp.sum(values, axis=-1, keepdims=True)


def unit_rows(values):
    factor = lax.rsqrt(row_sum(values * values) + EPS)
    return (values * factor, factor)


def back_rows(normal, factor, upstream):
    return factor * (upstream - normal * row_sum(normal * upstream))


def next_chip(block):
    chips = lax.axis_size(DP) // 2
    route = [(2 * i + c, 2 * ((i + (1, -1)[c]) % chips) + c) for i in range(chips) for c in (0, 1)]
    return lax.ppermute(block, DP, route)


def other_core(block):
    return lax.ppermute(block, "c", [(0, 1), (1, 0)])


def in_hbm(array):
    return pltpu.with_memory_space_constraint(array, pltpu.HBM)


def cost(flops, nbytes):
    return pl.CostEstimate(flops=flops, bytes_accessed=nbytes, transcendentals=0)


def units_kernel(core_ref, image_hbm, feats_hbm, proj_hbm, *refs):
    refs = list(refs)
    per = image_hbm.shape[0] // PIECE
    streams, stills = refs[:per], refs[per : 2 * per]
    stream_ref, own_ref, cross_ref, image_ref, feats_ref, proj_ref, sems = refs[2 * per :]
    moves = [(image_hbm, image_ref), (feats_hbm, feats_ref), (proj_hbm, proj_ref)]
    copies = [
        [
            pltpu.make_async_copy(
                src.at[pl.ds(at, LOAD), :], dst.at[pl.ds(at, LOAD), :], sems.at[n, at // LOAD]
            )
            for at in range(0, src.shape[0], LOAD)
        ]
        for n, (src, dst) in enumerate(moves)
    ]
    for group in copies:
        for copy in group:
            copy.start()
    core = core_ref[0]
    for copy in copies[0]:
        copy.wait()
    blocks = [pl.ds(i * PIECE, PIECE) for i in range(per)]
    u = [unit_rows(image_ref[at, :].astype(F32))[0].astype(BF16) for at in blocks]
    for copy in copies[1] + copies[2]:
        copy.wait()
    for i, at in enumerate(blocks):
        image = image_ref[at, :].astype(F32)
        text = jnp.dot(feats_ref[at, :], proj_ref[...], preferred_element_type=F32)
        v = unit_rows(text)[0].astype(BF16)
        streams[i][...] = stream_ref[at, :] = jnp.where(core == 0, v, u[i])
        stills[i][...] = jnp.where(core == 0, u[i], v)
        own_ref[at, :] = jnp.where(core == 0, image, text)
        cross_ref[at, :] = jnp.where(core == 0, text, image)


def units(core, images, feats, proj):
    rows, (deep, width) = images.shape[0], proj.shape
    per = rows // PIECE
    shape = lambda n, dtype: jax.ShapeDtypeStruct((n, width), dtype)
    call = pl.pallas_call(
        units_kernel,
        out_shape=[shape(PIECE, BF16)] * (2 * per) + [shape(rows, BF16)] + [shape(rows, F32)] * 2,
        in_specs=[SCALARS] + [pl.BlockSpec(memory_space=pltpu.HBM)] * 3,
        out_specs=[CHIP] * (2 * per + 3),
        scratch_shapes=[
            pltpu.VMEM(images.shape, BF16),
            pltpu.VMEM(feats.shape, BF16),
            pltpu.VMEM((deep, width), BF16),
            pltpu.SemaphoreType.DMA((3, deep // LOAD)),
        ],
        compiler_params=LIMIT,
        cost_estimate=cost(2 * rows * deep * width, 4 << 20),
        name="units",
    )
    outs = list(call(core, *(in_hbm(a) for a in (images, feats, proj))))
    return outs[:per], outs[per : 2 * per], outs[2 * per :]


def weigh(scalars, logits, offset):
    scale, bias = scalars[0], scalars[1]
    logits = scale * logits + bias
    if offset is None:
        return (scale / (1.0 + jnp.exp(-logits))).astype(BF16)
    rows = lax.broadcasted_iota(jnp.int32, logits.shape, 0)
    cols = lax.broadcasted_iota(jnp.int32, logits.shape, 1)
    label = jnp.where(rows == cols + offset, 1.0, -1.0)
    return (-label * scale / (1.0 + jnp.exp(label * logits))).astype(BF16)


def tile_kernel(plan, fresh, final, scalars, still_ref, *refs):
    refs = list(refs)
    out_ref = refs.pop()
    raw_ref = refs.pop(0) if final else None
    sums_ref = None if fresh else refs.pop(0)
    rows = still_ref.shape[0] // 2
    for half, pieces in enumerate(plan):
        at = slice(half * rows, (half + 1) * rows)
        still = still_ref[at, :]
        product = lambda i: lax.dot_general(
            still, refs[i][...], (((1,), (1,)), ((), ())), preferred_element_type=F32
        )
        total = None if fresh else sums_ref[at, :]
        ready = product(pieces[0][0]) if pieces else None
        for n, (i, offset) in enumerate(pieces):
            logits = ready
            ready = product(pieces[n + 1][0]) if n + 1 < len(pieces) else None
            part = jnp.dot(
                weigh(scalars, logits, offset), refs[i][...], preferred_element_type=F32
            )
            total = part if total is None else total + part
        if final:
            normal, factor = unit_rows(raw_ref[at, :])
            total = back_rows(normal, factor, total).astype(BF16)
        out_ref[at, :] = total


def tiles(plan, scalars, still, held, sums=None, raw=None):
    rows, width = still.shape
    operands = [still] + ([] if raw is None else [raw]) + ([] if sums is None else [sums])
    operands += list(held)
    count = sum(len(p) for p in plan)
    return pl.pallas_call(
        functools.partial(tile_kernel, plan, sums is None, raw is not None),
        out_shape=jax.ShapeDtypeStruct((rows, width), F32 if raw is None else BF16),
        in_specs=[SCALARS] + [CHIP] * len(operands),
        out_specs=CHIP,
        compiler_params=LIMIT,
        cost_estimate=cost(2 * count * rows * PIECE * width, 1 << 20),
    )(scalars, *operands)


def pick_kernel(core_ref, own_hbm, sib_ref, out_ref, own_ref, sem):
    copy = pltpu.make_async_copy(own_hbm, own_ref, sem.at[0])
    copy.start()
    core = core_ref[0]
    rows, wide = own_ref.shape
    deep, plane = SIZES[2], SIZES[0] * SIZES[1] * SIZES[4]
    each = wide // (2 * deep * plane)
    shape = (wide, wide // 2)
    at = lax.broadcasted_iota(jnp.int32, shape, 1)
    j, z, p = at % each, (at // each) % deep, at // (each * deep)
    owner = (((p // 2) * deep + z) * 2 + core) * 2 + p % 2
    pick = jnp.where(
        lax.broadcasted_iota(jnp.int32, shape, 0) == owner * each + j, 1.0, 0.0
    ).astype(BF16)
    take = lambda ref: jnp.dot(ref[...], pick, preferred_element_type=F32).astype(BF16)
    sib = take(sib_ref)
    copy.wait()
    own = take(own_ref)

    @pl.when(core == 0)
    def _():
        out_ref[:rows, :], out_ref[rows:, :] = sib, own

    @pl.when(core != 0)
    def _():
        out_ref[:rows, :], out_ref[rows:, :] = own, sib


def pick_columns(core, own, sib):
    rows, wide = own.shape
    return pl.pallas_call(
        pick_kernel,
        out_shape=jax.ShapeDtypeStruct((2 * rows, wide // 2), BF16),
        in_specs=[SCALARS, pl.BlockSpec(memory_space=pltpu.HBM), CHIP],
        out_specs=CHIP,
        scratch_shapes=[pltpu.VMEM((rows, wide), BF16), pltpu.SemaphoreType.DMA((1,))],
        compiler_params=LIMIT,
        cost_estimate=cost(2 * rows * wide * wide, 2 << 20),
        name="pick",
    )(core, own, sib)


def proj_kernel(core_ref, feats_ref, mine_ref, crossed_ref, out_ref):
    def put(grads):
        out_ref[...] = lax.dot_general(
            feats_ref[...], grads, (((0,), (0,)), ((), ())), preferred_element_type=F32
        ).astype(BF16)

    @pl.when(core_ref[0] == 0)
    def _():
        put(crossed_ref[...])

    @pl.when(core_ref[0] != 0)
    def _():
        put(mine_ref[...])


def proj_part(core, feats, mine, crossed):
    depth, rows = feats.shape
    width = mine.shape[1]
    return pl.pallas_call(
        proj_kernel,
        out_shape=jax.ShapeDtypeStruct((rows, width), BF16),
        in_specs=[SCALARS] + [CHIP] * 3,
        out_specs=CHIP,
        compiler_params=LIMIT,
        cost_estimate=cost(2 * depth * rows * width, 1 << 20),
        name="proj",
    )(core, feats, mine, crossed)


def fold_kernel(parts_ref, out_ref):
    total = jnp.sum(parts_ref[...].astype(F32), axis=0)
    count, each, _ = out_ref.shape
    for i in range(count):
        out_ref[i, :, :] = total[i * each : (i + 1) * each, :]


def fold(parts, count):
    _, rows, width = parts.shape
    return pl.pallas_call(
        fold_kernel,
        out_shape=jax.ShapeDtypeStruct((count, rows // count, width), F32),
        in_specs=[CHIP],
        out_specs=CHIP,
        compiler_params=LIMIT,
        cost_estimate=cost(parts.size, 2 * parts.size),
        name="fold",
    )(parts)


def on_device(images, text_feats, text_proj, logit_scale, logit_bias):
    core_id = lax.axis_index("c").astype(jnp.int32)
    core = core_id.reshape(1)
    first = core_id == 0
    rows = images.shape[0]
    per = rows // PIECE
    scalars = jnp.concatenate([logit_scale, logit_bias])

    stream, still, (whole, raw, cross) = units(core, images, text_feats, text_proj)
    held = stream + [other_core(b) for b in still]
    moving = [next_chip(b) for b in held]
    still = jnp.concatenate(still + [other_core(whole)])
    raw = jnp.concatenate([raw, other_core(cross)])
    picked = pick_columns(core, text_feats, other_core(text_feats))

    pairs = lambda at: [(at + i, None) for i in range(per)]
    diagonal = [(i, i * PIECE) for i in range(per)]
    sums = tiles((diagonal, pairs(0)), scalars, still, held[:per])
    sums = tiles(([], diagonal), scalars, still, held[per:], sums)
    last = SHIFTS // 2
    for _ in range(1, last):
        held = moving
        moving = [next_chip(b) for b in held]
        sums = tiles((pairs(0), pairs(0)), scalars, still, held[:per], sums)
        sums = tiles((pairs(0), pairs(0)), scalars, still, held[per:], sums)
    sums = tiles((pairs(0), []), scalars, still, moving[:per], sums)
    one = [(0, None)]
    for b in moving[per:-1]:
        sums = tiles((one, one), scalars, still, [b], sums)
    grads = tiles((one, one), scalars, still, moving[-1:], sums, raw)

    crossed = other_core(grads)
    part = proj_part(core, picked, grads, crossed)
    image_grad = jnp.where(first, grads[:rows], crossed[rows:])
    plane, deep = lax.axis_size(PLANE), lax.axis_size("z")
    each = text_feats.shape[1] // (2 * plane * deep)
    part = part.reshape(plane, deep * each, -1)
    part = lax.all_to_all(part, PLANE, 0, 0, tiled=True)
    part = fold(part, deep)
    part = lax.all_to_all(part, "z", 0, 0, tiled=True)
    return (image_grad, jnp.sum(part, axis=0))


def solution(mesh):
    fine = Mesh(mesh.devices.reshape(SIZES), AXES)
    split = P(AXES, None)
    in_specs = (split, split, P(), P(), P())

    return jax.shard_map(
        on_device, mesh=fine, in_specs=in_specs, out_specs=(split, split), check_vma=False
    )
```
